32 devices in a mesh: pw: 2 (over x), pair: 16 (over z, y, core).
Axes of the slice: x: 2, y: 2, z: 4, core: 2. Of those that a mesh axis runs over, the one named last changes fastest.
Arguments:
- valence_pairs: bfloat16 [64, 64, 8192], P('pair', None, 'pw'), may hold values from -0.59765625 to 0.59765625
- conduction_pairs: bfloat16 [16, 256, 8192], P('pair', None, 'pw'), may hold values from -0.59765625 to 0.59765625
- screening: float32 [8192], P('pw'), may hold values from 0.1 to 2
Outputs:
- kernel: float32 [64, 16, 64, 256], P('pair', None, 'pw')
The draws below stay inside these ranges and needn't reach their ends.
All inputs are finite; a program needn't handle non-finite values.
Results may differ from the reference program's by a relative error of at most 0.0029.
Values may be sent and summed in bfloat16 or wider, within the bound.
A program may use at most 128 MiB of HBM per device.

```python
import math
import jax
import jax.numpy as jnp
from jax import lax

V = 64
C = 256
G = 8192
CS = 16


def raised(entries, own_key, source, target, shards_of, factor):
    owner, partner = [(jnp.arange(entries.shape[dim]) // (entries.shape[dim] // shards_of)).reshape([-1 if axis == dim else 1 for axis in range(entries.ndim)]) for dim in (source, target)]
    chosen = jax.random.permutation(own_key, shards_of)[partner]
    strong = (owner == chosen) | (owner == (partner + shards_of // 2) % shards_of)
    return jnp.where(strong, factor * entries, entries)


def levels(stream_key, shape, shards, least, largest):
    gain = 1.0
    for dim, parts in shards:
        draws = jax.random.uniform(jax.random.fold_in(jax.random.fold_in(stream_key, 6), dim), (parts,), jnp.float32, least / len(shards), largest / len(shards))
        gain = gain * jnp.repeat(jnp.exp(draws), shape[dim] // parts).reshape((-1,) + (1,) * (len(shape) - 1 - dim))
    return gain


def gaussian(rng, dims, spread, most, pieces=(), held_as=jnp.bfloat16):
    array = jax.random.normal(rng, dims, jnp.float32) * spread
    if len(pieces) > 0:
        array = levels(rng, dims, pieces, -0.22, 0.18) * array
    return jnp.clip(array, min=-most, max=most).astype(held_as)


def heavy_noise(key, dims, scale, limit, split, heavy, held_as=jnp.bfloat16):
    entries = scale * jax.random.normal(key, dims, jnp.float32)
    if split:
        entries = entries * levels(key, dims, split, -0.22, 0.18)
    return jnp.clip(raised(entries, jax.random.fold_in(key, 3), *heavy), -limit, limit).astype(held_as)


def setup_inputs(seed: int = 0) -> dict:
    streams_of = jax.random.split(jax.random.key(seed), 4)
    valence_pairs = heavy_noise(streams_of[0], (V, V, G), 0.1, 0.59765625, ((0, 16), (2, 2)), (2, 1, 2, 2.0))
    conduction_pairs = gaussian(streams_of[1], (CS, C, G), 0.1, 0.59765625, ((0, 16), (2, 2)))
    screening = jnp.clip(jnp.exp(math.log(2.0) - 2.9957323 * jax.random.uniform(streams_of[2], (G,), jnp.float32) ** levels(streams_of[2], (G,), ((0, 2),), -0.2, 0.2)), 0.1, 2.0)
    return {"valence_pairs": valence_pairs, "conduction_pairs": conduction_pairs, "screening": screening}


def reference(valence_pairs, conduction_pairs, screening):
    screened = (valence_pairs.astype(jnp.float32) * screening[None, None, :]).astype(jnp.bfloat16)
    left = screened.astype(jnp.float32).reshape(V * V, G)
    right = conduction_pairs.astype(jnp.float32).reshape(CS * C, G)
    product = lax.dot_general(left, right, (((1,), (1,)), ((), ())), preferred_element_type=jnp.float32)
    return product.reshape(V, V, CS, C).transpose(0, 2, 1, 3)
```

```python
import functools

import jax
import jax.numpy as jnp
from jax import lax
from jax.experimental import pallas as pl
from jax.experimental.pallas import tpu as pltpu
from jax.sharding import PartitionSpec as P

MESH = pl.DeviceIdType.MESH
SIDE = 4
CHUNKS = 16
BLOCKS = 5
PARTS = 2


def contract(piece, flat_right, band_dev, conduction):
    first, second, width = piece.shape
    product = lax.dot_general(
        piece.reshape(first * second, width),
        flat_right,
        (((1,), (1,)), ((), ())),
        preferred_element_type=jnp.float32,
    )
    return product.reshape(first, second, band_dev, conduction)


def general_body(valence_pairs, conduction_pairs, screening):
    screened = (valence_pairs.astype(jnp.float32) * screening[None, None, :]).astype(jnp.bfloat16)
    band_dev, conduction, plane_dev = conduction_pairs.shape
    flat_local = conduction_pairs.reshape(band_dev * conduction, plane_dev)
    partial_value = contract(
        lax.all_gather(screened, "pair", axis=0, tiled=True), flat_local, band_dev, conduction
    )
    terms = lax.psum_scatter(partial_value, "pw", scatter_dimension=1, tiled=True)
    owned = lax.all_to_all(terms, "pair", split_axis=0, concat_axis=2, tiled=True)
    return owned.transpose(0, 2, 1, 3)


def flip(bit, by):
    return bit + by - 2 * bit * by


def grid_kernel(
    val, con, scr_row, out, raw, scr, bb, acc, xs, xr, zs, zr,
    loc, a1s, a1r, a2s, a2r, a3s, a3r, b1s, b1r, b2s, b2r, b3s, b3r, b4s, b4r, xss, xsr, zss, zsr,
):
    me, x = lax.axis_index("pair"), lax.axis_index("pw")
    core, y, zl, zh = me % 2, (me // 2) % 2, (me // 4) % 2, me // 8
    rows, depth = val.shape
    cols = con.shape[0]
    half = out.shape[2]
    vb, w, part = acc.shape[1], acc.shape[2], acc.shape[3]
    step = rows // CHUNKS
    cstep = cols // CHUNKS
    end = zl == zh
    mid = zl != zh

    def at(fc, fy, fl, fh):
        return (x, flip(core, fc) + 2 * flip(y, fy) + 4 * flip(zl, fl) + 8 * flip(zh, fh))

    def remote(src, dst, s, r, dev):
        return pltpu.make_async_remote_copy(
            src_ref=src, dst_ref=dst, send_sem=s, recv_sem=r, device_id=dev, device_id_type=MESH
        )

    def arows(k):
        return pl.ds(pl.multiple_of(k * step, step), step)

    def brows(k):
        return pl.ds(pl.multiple_of(k * cstep, cstep), cstep)

    sibling, beside, near, far = at(1, 0, 0, 0), at(0, 1, 0, 0), at(0, 0, 1, 0), at(0, 0, 0, 1)
    across = at(0, 0, 1, 1)
    a1 = remote(raw.at[0], raw.at[1], a1s.at[0], a1r.at[0], sibling)
    b1 = remote(bb.at[0], bb.at[1], b1s.at[0], b1r.at[0], beside)

    def a2(k):
        return remote(raw.at[0, arows(k)], raw.at[2, arows(k)], a2s.at[k], a2r.at[k], near)

    def a3(k):
        return remote(raw.at[2, arows(k)], raw.at[3, arows(k)], a3s.at[k], a3r.at[k], sibling)

    def b2(k):
        return remote(bb.at[0, brows(k)], bb.at[2, brows(k)], b2s.at[k], b2r.at[k], far)

    def b2pass(k):
        return remote(bb.at[4, brows(k)], bb.at[2, brows(k)], b2s.at[k], b2r.at[k], near)

    def b3(k):
        return remote(bb.at[2, brows(k)], bb.at[3, brows(k)], b3s.at[k], b3r.at[k], beside)

    def b4(k):
        return remote(bb.at[0, brows(k)], bb.at[4, brows(k)], b4s.at[k], b4r.at[k], across)

    def slot(a, b, h):
        return (b * SIDE + a) * PARTS + h

    def xcopy(t):
        return remote(xs.at[t], xr.at[t], xss.at[t], xsr.at[t], (1 - x, me))

    def zcopy(t, a):
        return remote(zs.at[t], zr.at[t], zss.at[t], zsr.at[t], at(a % 2, 0, a // 2, 0))

    def each(n, fn, lo=0):
        def run(k, carry):
            fn(k)
            return carry
        lax.fori_loop(lo, n, run, 0)

    def active(a, b):
        kept = jnp.logical_and(b == 4, jnp.logical_and(mid, a < 2))
        shared = jnp.logical_and(b == 2, jnp.logical_or(mid, a < 2))
        return jnp.logical_or(jnp.logical_or(kept, shared), jnp.logical_and(b != 2, b != 4))

    def returned(a, b):
        kept = jnp.logical_and(b == 4, jnp.logical_and(mid, a < 2))
        shared = jnp.logical_and(b == 2, jnp.logical_or(end, a < 2))
        return jnp.logical_or(jnp.logical_or(kept, shared), jnp.logical_and(b != 2, b != 4))

    def owner(a, b):
        fy = jnp.where(b == 4, 0, b % 2)
        fl = jnp.where(b == 4, 1, 0)
        fh = jnp.where(b >= 2, 1, 0)
        return (
            flip(core, a % 2) + 2 * flip(y, fy) + 4 * flip(flip(zl, a // 2), fl) + 8 * flip(zh, fh)
        )

    barrier = pltpu.get_barrier_semaphore()
    greeted = (sibling, beside, near, far, at(1, 0, 1, 0), (1 - x, me), across)
    for dev in greeted:
        pl.semaphore_signal(barrier, inc=1, device_id=dev, device_id_type=MESH)
    own_a = pltpu.make_async_copy(val, raw.at[0], loc.at[0])
    own_b = pltpu.make_async_copy(con, bb.at[0], loc.at[1])
    own_a.start()
    own_b.start()
    own_a.wait()
    own_b.wait()
    pl.semaphore_wait(barrier, len(greeted))

    @pl.when(mid)
    def _():
        each(CHUNKS, lambda k: b4(k).start())

    each(CHUNKS, lambda k: a2(k).start())

    @pl.when(end)
    def _():
        each(CHUNKS, lambda k: b2(k).start())

    b1.start()
    a1.start()

    lines = 16

    def screen(a, r):
        scr[a, r, :] = (raw[a, r, :].astype(jnp.float32) * scr_row[...]).astype(jnp.bfloat16)

    def screen_all(a):
        each(rows // lines, lambda i: screen(a, pl.ds(pl.multiple_of(i * lines, lines), lines)))

    def compute(a, b, h):
        @pl.when(active(a, b))
        def _():
            t = slot(a, b, h)
            right = bb[b, pl.ds(pl.multiple_of(h * part, part), part), :]
            prod = lax.dot_general(
                scr[a], right, (((1,), (1,)), ((), ())), preferred_element_type=jnp.float32
            )
            acc[t] = prod.reshape(vb, w, part)
            other = pl.ds(pl.multiple_of((1 - x) * half, half), half)
            xs[t] = acc[t, :, other, :].astype(jnp.bfloat16)
            xcopy(t).start()

    def place(a, b, h, value):
        lanes = pl.ds(pl.multiple_of(h * part, part), part)
        out[:, pl.ds(owner(a, b), 1), :, lanes] = value[:, None]

    def drain(a, b, h):
        @pl.when(active(a, b))
        def _():
            t = slot(a, b, h)
            xcopy(t).wait_recv()
            mine = pl.ds(pl.multiple_of(x * half, half), half)
            total = acc[t, :, mine, :] + xr[t].astype(jnp.float32)

            @pl.when(a == 0)
            def _():
                place(0, b, h, total)

            @pl.when(a > 0)
            def _():
                zs[t] = total.astype(jnp.bfloat16)
                zcopy(t, a).start()

    def land(a, b, h):
        @pl.when(returned(a, b))
        def _():
            t = slot(a, b, h)
            zcopy(t, a).wait_recv()
            place(a, b, h, zr[t].astype(jnp.float32))

    screen_all(0)
    each(PARTS, lambda h: compute(0, 0, h))
    a1.wait_recv()
    screen_all(1)
    each(PARTS, lambda h: compute(1, 0, h))

    def first(k):
        @pl.when(mid)
        def _():
            b4(k).wait_recv()
            b2pass(k).start()

        a2(k).wait_recv()
        a3(k).start()
        screen(2, arows(k))

        @pl.when(k > 0)
        def _():
            a3(k - 1).wait_recv()
            screen(3, arows(k - 1))

    each(CHUNKS, first)
    a3(CHUNKS - 1).wait_recv()
    screen(3, arows(CHUNKS - 1))
    each(PARTS * 2, lambda i: drain(1 - i // PARTS, 0, i % PARTS))
    b1.wait_recv()

    turns = CHUNKS // 2

    def early(i):
        j = i - 2
        a = jnp.where(i < 2, i, jnp.where(j < 2, 2 + j, j - 2))
        b = jnp.where(i < 2, 4, jnp.where(j < 2, 0, 1))
        return a, b

    def relay(k):
        b2(k).wait_recv()
        b3(k).start()

    def second(k):
        relay(k)
        a, b = early(k)
        each(PARTS, lambda h: compute(a, b, h))

        @pl.when(k > 0)
        def _():
            pa, pb = early(k - 1)
            each(PARTS, lambda h: drain(pa, pb, h))

    each(turns, second)

    def late(i):
        return SIDE - 1 - i % SIDE, 2 + i // SIDE

    def third(k):
        relay(k + turns)

        @pl.when(k == 0)
        def _():
            pa, pb = early(turns - 1)
            each(PARTS, lambda h: drain(pa, pb, h))

        @pl.when(k == SIDE)
        def _():
            each(turns, lambda i: b3(i).wait_recv())

        a, b = late(k)
        compute(a, b, 0)

        @pl.when(k > 0)
        def _():
            pa, pb = late(k - 1)
            drain(pa, pb, 0)

    each(turns, third)

    def last(k):
        @pl.when(k == SIDE)
        def _():
            each(CHUNKS, lambda i: b3(i).wait_recv(), turns)

        a, b = late(k)
        compute(a, b, 1)

        @pl.when(k == 0)
        def _():
            pa, pb = late(turns - 1)
            drain(pa, pb, 0)

        @pl.when(k > 1)
        def _():
            pa, pb = late(k - 2)
            drain(pa, pb, 1)

    each(turns, last)

    def finish(k):
        pa, pb = late(k)
        drain(pa, pb, 1)

    each(turns, finish, turns - 2)

    def arrive(i):
        h = i // (BLOCKS * (SIDE - 1))
        j = i % (BLOCKS * (SIDE - 1))
        land(1 + j % (SIDE - 1), j // (SIDE - 1), h)

    each(PARTS * BLOCKS * (SIDE - 1), arrive)

    a1.wait_send()
    b1.wait_send()

    def sent(k):
        a2(k).wait_send()
        a3(k).wait_send()
        b2(k).wait_send()
        b3(k).wait_send()

        @pl.when(mid)
        def _():
            b4(k).wait_send()
    each(CHUNKS, sent)

    def passed(i):
        a, b, h = (i // PARTS) % SIDE, i // (PARTS * SIDE), i % PARTS

        @pl.when(active(a, b))
        def _():
            xcopy(i).wait_send()

            @pl.when(a > 0)
            def _():
                zcopy(i, a).wait_send()
    each(BLOCKS * SIDE * PARTS, passed)


def grid_body(valence_pairs, conduction_pairs, screening):
    vb, w, depth = valence_pairs.shape
    bands, conduction, _ = conduction_pairs.shape
    cols = bands * conduction
    rows = vb * w
    half = w // lax.axis_size("pw")
    total_c = bands * lax.axis_size("pair")
    tiles = BLOCKS * SIDE * PARTS
    part = cols // PARTS
    dma = pltpu.SemaphoreType.DMA
    bf16 = jnp.bfloat16
    return pl.pallas_call(
        grid_kernel,
        out_shape=jax.ShapeDtypeStruct((vb, total_c, half, conduction), jnp.float32),
        in_specs=[
            pl.BlockSpec(memory_space=pl.ANY),
            pl.BlockSpec(memory_space=pl.ANY),
            pl.BlockSpec(memory_space=pltpu.VMEM),
        ],
        out_specs=pl.BlockSpec(memory_space=pltpu.VMEM),
        scratch_shapes=[
            pltpu.VMEM((SIDE, rows, depth), bf16),
            pltpu.VMEM((SIDE, rows, depth), bf16),
            pltpu.VMEM((BLOCKS, cols, depth), bf16),
            pltpu.VMEM((tiles, vb, w, part), jnp.float32),
            pltpu.VMEM((tiles, vb, half, part), bf16),
            pltpu.VMEM((tiles, vb, half, part), bf16),
            pltpu.VMEM((tiles, vb, half, part), bf16),
            pltpu.VMEM((tiles, vb, half, part), bf16),
            dma((2,)),
            dma((1,)), dma((1,)),
            dma((CHUNKS,)), dma((CHUNKS,)), dma((CHUNKS,)), dma((CHUNKS,)),
            dma((1,)), dma((1,)),
            dma((CHUNKS,)), dma((CHUNKS,)), dma((CHUNKS,)), dma((CHUNKS,)),
            dma((CHUNKS,)), dma((CHUNKS,)),
            dma((tiles,)), dma((tiles,)), dma((tiles,)), dma((tiles,)),
        ],
        compiler_params=pltpu.CompilerParams(
            collective_id=0, has_side_effects=True, vmem_limit_bytes=56 * 1024 * 1024
        ),
    )(
        valence_pairs.reshape(rows, depth),
        conduction_pairs.reshape(cols, depth),
        screening.reshape(1, depth),
    )


def solution(mesh):
    placed = (P("pair", None, "pw"), P("pair", None, "pw"), P("pw"))
    squared = mesh.shape["pw"] == 2 and mesh.shape["pair"] == SIDE * SIDE

    def body(valence_pairs, conduction_pairs, screening):
        if squared and conduction_pairs.shape[0] == 1:
            return grid_body(valence_pairs, conduction_pairs, screening)
        return general_body(valence_pairs, conduction_pairs, screening)

    return jax.shard_map(
        body, mesh=mesh, in_specs=placed, out_specs=P("pair", None, "pw", None), check_vma=False
    )
```

```python
import functools

import jax
import jax.numpy as jnp
from jax import lax
from jax.experimental import pallas as pl
from jax.experimental.pallas import tpu as pltpu
from jax.sharding import PartitionSpec as P

MESH = pl.DeviceIdType.MESH
SIDE = 4
CHUNKS = 8
BLOCKS = 5
CUTS = 8
PARTS = 2


def contract(piece, flat_right, band_dev, conduction):
    first, second, width = piece.shape
    product = lax.dot_general(
        piece.reshape(first * second, width),
        flat_right,
        (((1,), (1,)), ((), ())),
        preferred_element_type=jnp.float32,
    )
    return product.reshape(first, second, band_dev, conduction)


def general_body(valence_pairs, conduction_pairs, screening):
    screened = (valence_pairs.astype(jnp.float32) * screening[None, None, :]).astype(jnp.bfloat16)
    band_dev, conduction, plane_dev = conduction_pairs.shape
    flat_local = conduction_pairs.reshape(band_dev * conduction, plane_dev)
    partial_value = contract(
        lax.all_gather(screened, "pair", axis=0, tiled=True), flat_local, band_dev, conduction
    )
    terms = lax.psum_scatter(partial_value, "pw", scatter_dimension=1, tiled=True)
    owned = lax.all_to_all(terms, "pair", split_axis=0, concat_axis=2, tiled=True)
    return owned.transpose(0, 2, 1, 3)


def flip(bit, by):
    return bit + by - 2 * bit * by


def grid_kernel(
    val, con, scr_row, out, raw, scr, bb, acc, xs, xr, zs, zr,
    loc, a1s, a1r, a2s, a2r, a3s, a3r, b1s, b1r, b2s, b2r, b3s, b3r, b4s, b4r, gate, xss, xsr, zss, zsr,
):
    me, x = lax.axis_index("pair"), lax.axis_index("pw")
    core, y, zl, zh = me % 2, (me // 2) % 2, (me // 4) % 2, me // 8
    rows, depth = val.shape
    cols = con.shape[0]
    half = out.shape[2]
    vb, w, part = acc.shape[1], acc.shape[2], acc.shape[3]
    step = rows // CHUNKS
    cstep = cols // CHUNKS
    cut = depth // CUTS
    bits = PARTS * CUTS
    end = zl == zh
    mid = zl != zh

    def at(fc, fy, fl, fh):
        return (x, flip(core, fc) + 2 * flip(y, fy) + 4 * flip(zl, fl) + 8 * flip(zh, fh))

    def remote(src, dst, s, r, dev):
        return pltpu.make_async_remote_copy(
            src_ref=src, dst_ref=dst, send_sem=s, recv_sem=r, device_id=dev, device_id_type=MESH
        )

    def arows(k):
        return pl.ds(pl.multiple_of(k * step, step), step)

    def brows(k):
        return pl.ds(pl.multiple_of(k * cstep, cstep), cstep)

    sibling, beside, near = at(1, 0, 0, 0), at(0, 1, 0, 0), at(0, 0, 1, 0)
    far, across = at(0, 0, 0, 1), at(0, 0, 1, 1)
    a1 = remote(raw.at[0], raw.at[1], a1s.at[0], a1r.at[0], sibling)

    def b1(k):
        return remote(bb.at[0, brows(k)], bb.at[1, brows(k)], b1s.at[k], b1r.at[k], beside)

    def a2(k):
        return remote(raw.at[0, arows(k)], raw.at[2, arows(k)], a2s.at[k], a2r.at[k], near)

    def a3(k):
        return remote(raw.at[2, arows(k)], raw.at[3, arows(k)], a3s.at[k], a3r.at[k], sibling)

    def bit(b, k):
        lines = pl.ds(pl.multiple_of((k // CUTS) * part, part), part)
        lanes = pl.ds(pl.multiple_of((k % CUTS) * cut, cut), cut)
        return bb.at[b, lines, lanes]

    def b2(k):
        return remote(bit(0, k), bit(2, k), b2s.at[k], b2r.at[k], far)

    def b2pass(k):
        return remote(bit(4, k), bit(2, k), b2s.at[k], b2r.at[k], near)

    def b3(k):
        return remote(bit(2, k), bit(3, k), b3s.at[k], b3r.at[k], beside)

    def b4(k):
        return remote(bb.at[0, brows(k)], bb.at[4, brows(k)], b4s.at[k], b4r.at[k], across)

    def slot(a, b, h):
        return (b * SIDE + a) * PARTS + h

    def xcopy(t):
        return remote(xs.at[t], xr.at[t], xss.at[t], xsr.at[t], (1 - x, me))

    def zcopy(t, a):
        return remote(zs.at[t], zr.at[t], zss.at[t], zsr.at[t], at(a % 2, 0, a // 2, 0))

    def each(n, fn, lo=0):
        def run(k, carry):
            fn(k)
            return carry
        lax.fori_loop(lo, n, run, 0)

    def active(a, b):
        kept = jnp.logical_and(b == 4, jnp.logical_and(mid, a < 2))
        shared = jnp.logical_and(b == 2, jnp.logical_or(mid, a < 2))
        return jnp.logical_or(jnp.logical_or(kept, shared), jnp.logical_and(b != 2, b != 4))

    def returned(a, b):
        kept = jnp.logical_and(b == 4, jnp.logical_and(mid, a < 2))
        shared = jnp.logical_and(b == 2, jnp.logical_or(end, a < 2))
        return jnp.logical_or(jnp.logical_or(kept, shared), jnp.logical_and(b != 2, b != 4))

    def owner(a, b):
        fy = jnp.where(b == 4, 0, b % 2)
        fl = jnp.where(b == 4, 1, 0)
        fh = jnp.where(b >= 2, 1, 0)
        return (
            flip(core, a % 2) + 2 * flip(y, fy) + 4 * flip(flip(zl, a // 2), fl) + 8 * flip(zh, fh)
        )

    lines = 16

    def screen(a, r):
        scr[a, r, :] = (raw[a, r, :].astype(jnp.float32) * scr_row[...]).astype(jnp.bfloat16)

    def blank(t):
        acc[t] = jnp.zeros((vb, w, part), jnp.float32)

    def screen_all(a):
        each(rows // lines, lambda i: screen(a, pl.ds(pl.multiple_of(i * lines, lines), lines)))

    barrier = pltpu.get_barrier_semaphore()
    greeted = (near, beside, (1 - x, me), sibling)

    @pl.when(mid)
    def _():
        pl.semaphore_signal(barrier, inc=1, device_id=across, device_id_type=MESH)

    for dev in greeted:
        pl.semaphore_signal(barrier, inc=1, device_id=dev, device_id_type=MESH)
    own_a = pltpu.make_async_copy(val, raw.at[0], loc.at[0])
    own_b = pltpu.make_async_copy(con, bb.at[0], loc.at[1])
    own_a.start()
    own_b.start()
    own_a.wait()
    screen_all(0)
    own_b.wait()
    each(2 * SIDE * PARTS, lambda i: blank(2 * SIDE * PARTS + i))
    pl.semaphore_wait(barrier, len(greeted) + jnp.where(mid, 1, 0))

    @pl.when(mid)
    def _():
        each(CHUNKS, lambda k: b4(k).start())

    each(CHUNKS, lambda k: a2(k).start())

    each(CHUNKS, lambda k: b1(k).start())
    a1.start()

    def send(a, b, h):
        @pl.when(active(a, b))
        def _():
            t = slot(a, b, h)
            other = pl.ds(pl.multiple_of((1 - x) * half, half), half)
            xs[t] = acc[t, :, other, :].astype(jnp.bfloat16)
            xcopy(t).start()

    def whole(a, b):
        @pl.when(active(a, b))
        def _():
            prod = lax.dot_general(
                scr[a], bb[b], (((1,), (1,)), ((), ())), preferred_element_type=jnp.float32
            )
            for h in range(PARTS):
                acc[slot(a, b, h)] = prod[:, h * part:(h + 1) * part].reshape(vb, w, part)
        each(PARTS, lambda h: send(a, b, h))

    def grow(b, k):
        h, q = k // CUTS, k % CUTS
        lanes = pl.ds(pl.multiple_of(q * cut, cut), cut)
        lines = pl.ds(pl.multiple_of(h * part, part), part)

        def one(i):
            a = SIDE - 1 - i

            @pl.when(active(a, b))
            def _():
                prod = lax.dot_general(
                    scr[a, :, lanes], bb[b, lines, lanes],
                    (((1,), (1,)), ((), ())), preferred_element_type=jnp.float32,
                )
                t = slot(a, b, h)
                acc[t] = acc[t] + prod.reshape(vb, w, part)

            @pl.when(q == CUTS - 1)
            def _():
                send(a, b, h)

        each(SIDE, one)

    def place(a, b, h, value):
        lanes = pl.ds(pl.multiple_of(h * part, part), part)
        out[:, pl.ds(owner(a, b), 1), :, lanes] = value[:, None]

    def drain(a, b, h):
        @pl.when(active(a, b))
        def _():
            t = slot(a, b, h)
            xcopy(t).wait_recv()
            mine = pl.ds(pl.multiple_of(x * half, half), half)
            total = acc[t, :, mine, :] + xr[t].astype(jnp.float32)

            @pl.when(a == 0)
            def _():
                place(0, b, h, total)

            @pl.when(a > 0)
            def _():
                zs[t] = total.astype(jnp.bfloat16)
                zcopy(t, a).start()

    def land(a, b, h):
        @pl.when(returned(a, b))
        def _():
            t = slot(a, b, h)
            zcopy(t, a).wait_recv()
            place(a, b, h, zr[t].astype(jnp.float32))

    whole(0, 0)
    a1.wait_recv()
    screen_all(1)
    whole(1, 0)

    ready = CHUNKS // PARTS

    def first(k):
        @pl.when(jnp.logical_and(mid, k == CHUNKS - 1))
        def _():
            each(CHUNKS, lambda i: b4(i).wait_send())
            for dev in (near, at(1, 0, 1, 0)):
                pl.semaphore_signal(gate, inc=1, device_id=dev, device_id_type=MESH)

        @pl.when(jnp.logical_and(end, k == CHUNKS - 1))
        def _():
            pl.semaphore_wait(gate, 2)
            each(bits, lambda i: b2(i).start())

        a2(k).wait_recv()
        a3(k).start()

        @pl.when(mid)
        def _():
            b4(k).wait_recv()

            @pl.when(k % ready == ready - 1)
            def _():
                each(CUTS, lambda i: b2pass((k // ready) * CUTS + i).start())

        screen(2, arows(k))

        @pl.when(k > 0)
        def _():
            a3(k - 1).wait_recv()
            screen(3, arows(k - 1))

    each(CHUNKS, first)
    a3(CHUNKS - 1).wait_recv()
    screen(3, arows(CHUNKS - 1))
    each(PARTS * 2, lambda i: drain(1 - i // PARTS, 0, i % PARTS))
    each(CHUNKS, lambda k: b1(k).wait_recv())

    turns = 2 * SIDE
    lag = 2

    def early(i):
        j = i - 2
        a = jnp.where(i < 2, i, jnp.where(j < 2, 2 + j, j - 2))
        b = jnp.where(i < 2, 4, jnp.where(j < 2, 0, 1))
        return a, b

    def between(lo, k, hi):
        return jnp.logical_and(k >= lo, k < hi)

    def tail(k):
        b3(k).wait_recv()
        grow(3, k)

    def second(k):
        b2(k).wait_recv()
        b3(k).start()
        grow(2, k)

        @pl.when(k < turns)
        def _():
            whole(*early(k))

        @pl.when(k >= lag)
        def _():
            tail(k - lag)

        @pl.when(between(lag, k, turns + lag))
        def _():
            a, b = early(k - lag)
            each(PARTS, lambda h: drain(a, b, h))

        @pl.when(between(CUTS + lag, k, CUTS + lag + SIDE))
        def _():
            drain(SIDE - 1 - (k - CUTS - lag), 2, 0)

        @pl.when(k >= bits - SIDE)
        def _():
            drain(bits - 1 - k, 3, 0)

        @pl.when(k >= bits - 6)
        def _():
            i = k - bits + 6
            land(1, jnp.where(i < 4, i // 2, 4), i % 2)

    each(bits, second)
    tail(bits - 2)
    each(SIDE, lambda i: drain(SIDE - 1 - i, 2, 1))
    tail(bits - 1)

    def arrive(lo, h):
        def one(j):
            land(2 + j % 2, lo + j // 2, h)
        return one

    land(1, 2, 0)
    land(1, 3, 0)
    each(4, arrive(0, 0))
    each(4, arrive(0, 1))
    each(4, arrive(2, 0))
    each(SIDE, lambda i: drain(SIDE - 1 - i, 3, 1))
    land(1, 2, 1)
    each(4, arrive(2, 1))
    land(1, 3, 1)

    a1.wait_send()

    def sent(k):
        a2(k).wait_send()
        a3(k).wait_send()
        b1(k).wait_send()
    each(CHUNKS, sent)

    def cleared(k):
        b2(k).wait_send()
        b3(k).wait_send()
    each(bits, cleared)

    def passed(i):
        a, b, h = (i // PARTS) % SIDE, i // (PARTS * SIDE), i % PARTS

        @pl.when(active(a, b))
        def _():
            xcopy(i).wait_send()

            @pl.when(a > 0)
            def _():
                zcopy(i, a).wait_send()
    each(BLOCKS * SIDE * PARTS, passed)


def grid_body(valence_pairs, conduction_pairs, screening):
    vb, w, depth = valence_pairs.shape
    bands, conduction, _ = conduction_pairs.shape
    cols = bands * conduction
    rows = vb * w
    half = w // lax.axis_size("pw")
    total_c = bands * lax.axis_size("pair")
    tiles = BLOCKS * SIDE * PARTS
    part = cols // PARTS
    bits = PARTS * CUTS
    dma = pltpu.SemaphoreType.DMA
    bf16 = jnp.bfloat16
    return pl.pallas_call(
        grid_kernel,
        out_shape=pltpu.VMEM((vb, total_c, half, conduction), jnp.float32),
        in_specs=[
            pl.BlockSpec(memory_space=pl.ANY),
            pl.BlockSpec(memory_space=pl.ANY),
            pl.BlockSpec(memory_space=pltpu.VMEM),
        ],
        out_specs=pl.BlockSpec(memory_space=pltpu.VMEM),
        scratch_shapes=[
            pltpu.VMEM((SIDE, rows, depth), bf16),
            pltpu.VMEM((SIDE, rows, depth), bf16),
            pltpu.VMEM((BLOCKS, cols, depth), bf16),
            pltpu.VMEM((tiles, vb, w, part), jnp.float32),
            pltpu.VMEM((tiles, vb, half, part), bf16),
            pltpu.VMEM((tiles, vb, half, part), bf16),
            pltpu.VMEM((tiles, vb, half, part), bf16),
            pltpu.VMEM((tiles, vb, half, part), bf16),
            dma((2,)),
            dma((1,)), dma((1,)),
            dma((CHUNKS,)), dma((CHUNKS,)), dma((CHUNKS,)), dma((CHUNKS,)),
            dma((CHUNKS,)), dma((CHUNKS,)),
            dma((bits,)), dma((bits,)), dma((bits,)), dma((bits,)),
            dma((CHUNKS,)), dma((CHUNKS,)),
            pltpu.SemaphoreType.REGULAR,
            dma((tiles,)), dma((tiles,)), dma((tiles,)), dma((tiles,)),
        ],
        compiler_params=pltpu.CompilerParams(
            collective_id=0, has_side_effects=True, vmem_limit_bytes=56 * 1024 * 1024
        ),
    )(
        valence_pairs.reshape(rows, depth),
        conduction_pairs.reshape(cols, depth),
        screening.reshape(1, depth),
    )


def solution(mesh):
    placed = (P("pair", None, "pw"), P("pair", None, "pw"), P("pw"))
    squared = mesh.shape["pw"] == 2 and mesh.shape["pair"] == SIDE * SIDE

    def body(valence_pairs, conduction_pairs, screening):
        if squared and conduction_pairs.shape[0] == 1:
            return grid_body(valence_pairs, conduction_pairs, screening)
        return general_body(valence_pairs, conduction_pairs, screening)

    return jax.shard_map(
        body, mesh=mesh, in_specs=placed, out_specs=P("pair", None, "pw", None), check_vma=False
    )
```

```python
import functools

import jax
import jax.numpy as jnp
from jax import lax
from jax.experimental import pallas as pl
from jax.experimental.pallas import tpu as pltpu
from jax.sharding import PartitionSpec as P

MESH = pl.DeviceIdType.MESH
SIDE = 4
CHUNKS = 4
BLOCKS = 5
CUTS = 8
TWICE = 1
LAST = 16
PARTS = 2


def contract(piece, flat_right, band_dev, conduction):
    first, second, width = piece.shape
    product = lax.dot_general(
        piece.reshape(first * second, width),
        flat_right,
        (((1,), (1,)), ((), ())),
        preferred_element_type=jnp.float32,
    )
    return product.reshape(first, second, band_dev, conduction)


def general_body(valence_pairs, conduction_pairs, screening):
    screened = (valence_pairs.astype(jnp.float32) * screening[None, None, :]).astype(jnp.bfloat16)
    band_dev, conduction, plane_dev = conduction_pairs.shape
    flat_local = conduction_pairs.reshape(band_dev * conduction, plane_dev)
    partial_value = contract(
        lax.all_gather(screened, "pair", axis=0, tiled=True), flat_local, band_dev, conduction
    )
    terms = lax.psum_scatter(partial_value, "pw", scatter_dimension=1, tiled=True)
    owned = lax.all_to_all(terms, "pair", split_axis=0, concat_axis=2, tiled=True)
    return owned.transpose(0, 2, 1, 3)


def flip(bit, by):
    return bit + by - 2 * bit * by


def grid_kernel(
    val, con, scr_in, out, scr_row, raw, scr, bb, acc, xs, xr, zs, zr,
    loc, a1s, a1r, a2s, a2r, a3s, a3r, b1s, b1r, b2s, b2r, b3s, b3r, b4s, b4r, b5s, gate, xss, xsr, zss, zsr,
):
    me, x = lax.axis_index("pair"), lax.axis_index("pw")
    core, y, zl, zh = me % 2, (me // 2) % 2, (me // 4) % 2, me // 8
    rows, depth = val.shape
    cols = con.shape[0]
    half = out.shape[2]
    vb, w, part = acc.shape[1], acc.shape[2], acc.shape[3]
    step = rows // CHUNKS
    cstep = cols // CHUNKS
    cut = depth // CUTS
    bits = PARTS * CUTS
    end = zl == zh
    mid = zl != zh

    def at(fc, fy, fl, fh):
        return (x, flip(core, fc) + 2 * flip(y, fy) + 4 * flip(zl, fl) + 8 * flip(zh, fh))

    def remote(src, dst, s, r, dev):
        return pltpu.make_async_remote_copy(
            src_ref=src, dst_ref=dst, send_sem=s, recv_sem=r, device_id=dev, device_id_type=MESH
        )

    def arows(k):
        return pl.ds(pl.multiple_of(k * step, step), step)

    def brows(k):
        return pl.ds(pl.multiple_of(k * cstep, cstep), cstep)

    sibling, beside, near = at(1, 0, 0, 0), at(0, 1, 0, 0), at(0, 0, 1, 0)
    far, across = at(0, 0, 0, 1), at(0, 0, 1, 1)
    a1 = remote(raw.at[0], raw.at[1], a1s.at[0], a1r.at[0], sibling)

    def b1(k):
        return remote(bb.at[0, brows(k)], bb.at[1, brows(k)], b1s.at[k], b1r.at[k], beside)

    def a2(k):
        return remote(raw.at[0, arows(k)], raw.at[2, arows(k)], a2s.at[k], a2r.at[k], near)

    def a3(k):
        return remote(raw.at[2, arows(k)], raw.at[3, arows(k)], a3s.at[k], a3r.at[k], sibling)

    def bit(b, k):
        lines = pl.ds(pl.multiple_of((k // CUTS) * part, part), part)
        lanes = pl.ds(pl.multiple_of((k % CUTS) * cut, cut), cut)
        return bb.at[b, lines, lanes]

    def b2(k):
        return remote(bit(0, k), bit(2, k), b2s.at[k], b2r.at[k], far)

    def b2pass(k):
        return remote(bit(4, k), bit(2, k), b2s.at[k], b2r.at[k], near)

    def b3(k):
        return remote(bit(2, k), bit(3, k), b3s.at[k], b3r.at[k], beside)

    def b5(j):
        k = bits - TWICE + j
        return remote(bit(1, k), bit(3, k), b5s.at[j], b3r.at[k], far)

    def b4(k):
        return remote(bb.at[0, brows(k)], bb.at[4, brows(k)], b4s.at[k], b4r.at[k], across)

    def b4_end(i):
        low = cols - LAST
        lines = pl.ds(cols - cstep, cstep - LAST) if i == 0 else pl.ds(low, LAST)
        lanes = pl.ds(0, depth) if i == 0 else pl.ds((i - 1) * (depth // 2), depth // 2)
        t = CHUNKS - 1 + i
        return remote(bb.at[0, lines, lanes], bb.at[4, lines, lanes], b4s.at[t], b4r.at[t], across)

    def slot(a, b, h):
        return (b * SIDE + a) * PARTS + h

    def xcopy(t):
        return remote(xs.at[t], xr.at[t], xss.at[t], xsr.at[t], (1 - x, me))

    def zcopy(t, a):
        return remote(zs.at[t], zr.at[t], zss.at[t], zsr.at[t], at(a % 2, 0, a // 2, 0))

    def each(n, fn, lo=0):
        def run(k, carry):
            fn(k)
            return carry
        lax.fori_loop(lo, n, run, 0)

    def active(a, b):
        kept = jnp.logical_and(b == 4, jnp.logical_and(mid, a < 2))
        shared = jnp.logical_and(b == 2, jnp.logical_or(mid, a < 2))
        return jnp.logical_or(jnp.logical_or(kept, shared), jnp.logical_and(b != 2, b != 4))

    def returned(a, b):
        kept = jnp.logical_and(b == 4, jnp.logical_and(mid, a < 2))
        shared = jnp.logical_and(b == 2, jnp.logical_or(end, a < 2))
        return jnp.logical_or(jnp.logical_or(kept, shared), jnp.logical_and(b != 2, b != 4))

    def owner(a, b):
        fy = jnp.where(b == 4, 0, b % 2)
        fl = jnp.where(b == 4, 1, 0)
        fh = jnp.where(b >= 2, 1, 0)
        return (
            flip(core, a % 2) + 2 * flip(y, fy) + 4 * flip(flip(zl, a // 2), fl) + 8 * flip(zh, fh)
        )

    lines = 16

    def screen(a, r):
        scr[a, r, :] = (raw[a, r, :].astype(jnp.float32) * scr_row[...]).astype(jnp.bfloat16)

    def blank(t):
        acc[t] = jnp.zeros((vb, w, part), jnp.float32)

    def screen_all(a):
        each(rows // lines, lambda i: screen(a, pl.ds(pl.multiple_of(i * lines, lines), lines)))

    barrier = pltpu.get_barrier_semaphore()
    greeted = (near, beside, (1 - x, me), sibling)

    @pl.when(mid)
    def _():
        pl.semaphore_signal(barrier, inc=1, device_id=across, device_id_type=MESH)

    for dev in greeted:
        pl.semaphore_signal(barrier, inc=1, device_id=dev, device_id_type=MESH)
    own_a = pltpu.make_async_copy(val, raw.at[0], loc.at[0])
    own_b = pltpu.make_async_copy(con, bb.at[0], loc.at[1])
    own_row = pltpu.make_async_copy(scr_in, scr_row, loc.at[2])
    own_row.start()
    own_a.start()
    own_b.start()
    own_row.wait()
    own_a.wait()
    screen_all(0)
    own_b.wait()
    each(2 * SIDE * PARTS, lambda i: blank(2 * SIDE * PARTS + i))
    pl.semaphore_wait(barrier, len(greeted) + jnp.where(mid, 1, 0))

    @pl.when(mid)
    def _():
        each(CHUNKS - 1, lambda k: b4(k).start())
        for i in range(3):
            b4_end(i).start()

    each(CHUNKS, lambda k: a2(k).start())

    each(CHUNKS, lambda k: b1(k).start())
    a1.start()

    def send(a, b, h):
        @pl.when(active(a, b))
        def _():
            t = slot(a, b, h)
            other = pl.ds(pl.multiple_of((1 - x) * half, half), half)
            xs[t] = acc[t, :, other, :].astype(jnp.bfloat16)
            xcopy(t).start()

    def whole(a, b):
        @pl.when(active(a, b))
        def _():
            prod = lax.dot_general(
                scr[a], bb[b], (((1,), (1,)), ((), ())), preferred_element_type=jnp.float32
            )
            for h in range(PARTS):
                acc[slot(a, b, h)] = prod[:, h * part:(h + 1) * part].reshape(vb, w, part)
        each(PARTS, lambda h: send(a, b, h))

    def grow(b, k):
        h, q = k // CUTS, k % CUTS
        lanes = pl.ds(pl.multiple_of(q * cut, cut), cut)
        lines = pl.ds(pl.multiple_of(h * part, part), part)

        def one(i):
            a = SIDE - 1 - i

            @pl.when(active(a, b))
            def _():
                prod = lax.dot_general(
                    scr[a, :, lanes], bb[b, lines, lanes],
                    (((1,), (1,)), ((), ())), preferred_element_type=jnp.float32,
                )
                t = slot(a, b, h)
                acc[t] = acc[t] + prod.reshape(vb, w, part)

            @pl.when(q == CUTS - 1)
            def _():
                send(a, b, h)

        each(SIDE, one)

    def place(a, b, h, value):
        lanes = pl.ds(pl.multiple_of(h * part, part), part)
        out[:, pl.ds(owner(a, b), 1), :, lanes] = value[:, None]

    def drain(a, b, h):
        @pl.when(active(a, b))
        def _():
            t = slot(a, b, h)
            xcopy(t).wait_recv()
            mine = pl.ds(pl.multiple_of(x * half, half), half)
            total = acc[t, :, mine, :] + xr[t].astype(jnp.float32)

            @pl.when(a == 0)
            def _():
                place(0, b, h, total)

            @pl.when(a > 0)
            def _():
                zs[t] = total.astype(jnp.bfloat16)
                zcopy(t, a).start()

    def land(a, b, h):
        @pl.when(returned(a, b))
        def _():
            t = slot(a, b, h)
            zcopy(t, a).wait_recv()
            place(a, b, h, zr[t].astype(jnp.float32))

    whole(0, 0)
    a1.wait_recv()
    screen_all(1)
    whole(1, 0)

    ready = CHUNKS // PARTS

    def first(k):
        @pl.when(jnp.logical_and(mid, k == CHUNKS - 1))
        def _():
            each(CHUNKS - 1, lambda i: b4(i).wait_send())
            b4_end(0).wait_send()
            b4_end(1).wait_send()
            for dev in (near, at(1, 0, 1, 0)):
                pl.semaphore_signal(gate, inc=1, device_id=dev, device_id_type=MESH)
            b4_end(2).wait_send()

        @pl.when(jnp.logical_and(end, k == CHUNKS - 1))
        def _():
            pl.semaphore_wait(gate, 2)
            each(bits, lambda i: b2(i).start())

        a2(k).wait_recv()
        a3(k).start()

        @pl.when(mid)
        def _():
            @pl.when(k < CHUNKS - 1)
            def _():
                b4(k).wait_recv()

            @pl.when(k == CHUNKS - 1)
            def _():
                for i in range(3):
                    b4_end(i).wait_recv()

            @pl.when(k % ready == ready - 1)
            def _():
                each(CUTS, lambda i: b2pass((k // ready) * CUTS + i).start())

        screen(2, arows(k))

        @pl.when(k > 0)
        def _():
            a3(k - 1).wait_recv()
            screen(3, arows(k - 1))

    each(CHUNKS, first)
    a3(CHUNKS - 1).wait_recv()
    screen(3, arows(CHUNKS - 1))
    each(PARTS * 2, lambda i: drain(1 - i // PARTS, 0, i % PARTS))
    each(CHUNKS, lambda k: b1(k).wait_recv())

    @pl.when(end)
    def _():
        each(TWICE, lambda j: b5(j).start())

    def crosses(k):
        return jnp.logical_or(end, k < bits - TWICE)

    turns = 2 * SIDE
    lag = 2

    def early(i):
        j = i - 2
        a = jnp.where(i < 2, i, jnp.where(j < 2, 2 + j, j - 2))
        b = jnp.where(i < 2, 4, jnp.where(j < 2, 0, 1))
        return a, b

    def between(lo, k, hi):
        return jnp.logical_and(k >= lo, k < hi)

    def tail(k):
        b3(k).wait_recv()
        grow(3, k)

    def second(k):
        b2(k).wait_recv()

        @pl.when(crosses(k))
        def _():
            b3(k).start()

        grow(2, k)

        @pl.when(k < turns)
        def _():
            whole(*early(k))

        @pl.when(k >= lag)
        def _():
            tail(k - lag)

        @pl.when(between(lag, k, turns + lag))
        def _():
            a, b = early(k - lag)
            each(PARTS, lambda h: drain(a, b, h))

        @pl.when(between(CUTS + lag, k, CUTS + lag + SIDE))
        def _():
            drain(SIDE - 1 - (k - CUTS - lag), 2, 0)

        @pl.when(k >= bits - SIDE)
        def _():
            drain(bits - 1 - k, 3, 0)

        @pl.when(k >= bits - 6)
        def _():
            i = k - bits + 6
            land(1, jnp.where(i < 4, i // 2, 4), i % 2)

    each(bits, second)
    tail(bits - 2)
    each(SIDE, lambda i: drain(SIDE - 1 - i, 2, 1))
    tail(bits - 1)

    def arrive(lo, h):
        def one(j):
            land(2 + j % 2, lo + j // 2, h)
        return one

    land(1, 2, 0)
    land(1, 3, 0)
    each(4, arrive(0, 0))
    each(4, arrive(0, 1))
    each(SIDE, lambda i: drain(SIDE - 1 - i, 3, 1))
    each(4, arrive(2, 0))
    land(1, 2, 1)
    each(4, arrive(2, 1))
    land(1, 3, 1)

    a1.wait_send()

    def sent(k):
        a2(k).wait_send()
        a3(k).wait_send()
        b1(k).wait_send()
    each(CHUNKS, sent)

    def cleared(k):
        b2(k).wait_send()

        @pl.when(crosses(k))
        def _():
            b3(k).wait_send()
    each(bits, cleared)

    @pl.when(end)
    def _():
        each(TWICE, lambda j: b5(j).wait_send())

    def passed(i):
        a, b, h = (i // PARTS) % SIDE, i // (PARTS * SIDE), i % PARTS

        @pl.when(active(a, b))
        def _():
            xcopy(i).wait_send()

            @pl.when(a > 0)
            def _():
                zcopy(i, a).wait_send()
    each(BLOCKS * SIDE * PARTS, passed)


def grid_body(valence_pairs, conduction_pairs, screening):
    vb, w, depth = valence_pairs.shape
    bands, conduction, _ = conduction_pairs.shape
    cols = bands * conduction
    rows = vb * w
    half = w // lax.axis_size("pw")
    total_c = bands * lax.axis_size("pair")
    tiles = BLOCKS * SIDE * PARTS
    part = cols // PARTS
    bits = PARTS * CUTS
    dma = pltpu.SemaphoreType.DMA
    bf16 = jnp.bfloat16
    return pl.pallas_call(
        grid_kernel,
        out_shape=pltpu.VMEM((vb, total_c, half, conduction), jnp.float32),
        in_specs=[
            pl.BlockSpec(memory_space=pl.ANY),
            pl.BlockSpec(memory_space=pl.ANY),
            pl.BlockSpec(memory_space=pl.ANY),
        ],
        out_specs=pl.BlockSpec(memory_space=pltpu.VMEM),
        scratch_shapes=[
            pltpu.VMEM((1, depth), jnp.float32),
            pltpu.VMEM((SIDE, rows, depth), bf16),
            pltpu.VMEM((SIDE, rows, depth), bf16),
            pltpu.VMEM((BLOCKS, cols, depth), bf16),
            pltpu.VMEM((tiles, vb, w, part), jnp.float32),
            pltpu.VMEM((tiles, vb, half, part), bf16),
            pltpu.VMEM((tiles, vb, half, part), bf16),
            pltpu.VMEM((tiles, vb, half, part), bf16),
            pltpu.VMEM((tiles, vb, half, part), bf16),
            dma((3,)),
            dma((1,)), dma((1,)),
            dma((CHUNKS,)), dma((CHUNKS,)), dma((CHUNKS,)), dma((CHUNKS,)),
            dma((CHUNKS,)), dma((CHUNKS,)),
            dma((bits,)), dma((bits,)), dma((bits,)), dma((bits,)),
            dma((CHUNKS + 2,)), dma((CHUNKS + 2,)),
            dma((TWICE,)),
            pltpu.SemaphoreType.REGULAR,
            dma((tiles,)), dma((tiles,)), dma((tiles,)), dma((tiles,)),
        ],
        compiler_params=pltpu.CompilerParams(
            collective_id=0, has_side_effects=True, vmem_limit_bytes=56 * 1024 * 1024
        ),
    )(
        valence_pairs.reshape(rows, depth),
        conduction_pairs.reshape(cols, depth),
        screening.reshape(1, depth),
    )


def solution(mesh):
    placed = (P("pair", None, "pw"), P("pair", None, "pw"), P("pw"))
    squared = mesh.shape["pw"] == 2 and mesh.shape["pair"] == SIDE * SIDE

    def body(valence_pairs, conduction_pairs, screening):
        if squared and conduction_pairs.shape[0] == 1:
            return grid_body(valence_pairs, conduction_pairs, screening)
        return general_body(valence_pairs, conduction_pairs, screening)

    return jax.shard_map(
        body, mesh=mesh, in_specs=placed, out_specs=P("pair", None, "pw", None), check_vma=False
    )
```

```python
import functools

import jax
import jax.numpy as jnp
from jax import lax
from jax.experimental import pallas as pl
from jax.experimental.pallas import tpu as pltpu
from jax.sharding import PartitionSpec as P

MESH = pl.DeviceIdType.MESH
SIDE = 4
CHUNKS = 4
BLOCKS = 5
CUTS = 8
TWICE = 1
LAST = 16
PARTS = 2


def contract(piece, flat_right, band_dev, conduction):
    first, second, width = piece.shape
    product = lax.dot_general(
        piece.reshape(first * second, width),
        flat_right,
        (((1,), (1,)), ((), ())),
        preferred_element_type=jnp.float32,
    )
    return product.reshape(first, second, band_dev, conduction)


def general_body(valence_pairs, conduction_pairs, screening):
    screened = (valence_pairs.astype(jnp.float32) * screening[None, None, :]).astype(jnp.bfloat16)
    band_dev, conduction, plane_dev = conduction_pairs.shape
    flat_local = conduction_pairs.reshape(band_dev * conduction, plane_dev)
    partial_value = contract(
        lax.all_gather(screened, "pair", axis=0, tiled=True), flat_local, band_dev, conduction
    )
    terms = lax.psum_scatter(partial_value, "pw", scatter_dimension=1, tiled=True)
    owned = lax.all_to_all(terms, "pair", split_axis=0, concat_axis=2, tiled=True)
    return owned.transpose(0, 2, 1, 3)


def flip(bit, by):
    return bit + by - 2 * bit * by


def grid_kernel(
    val, con, scr_in, out, scr_row, raw, scr, bb, acc, xs, xr, zs, zr,
    loc, a1s, a1r, a2s, a2r, a3s, a3r, b1s, b1r, b2s, b2r, b3s, b3r, b4s, b4r, b5s, gate, xss, xsr, zss, zsr,
):
    me, x = lax.axis_index("pair"), lax.axis_index("pw")
    core, y, zl, zh = me % 2, (me // 2) % 2, (me // 4) % 2, me // 8
    rows, depth = val.shape
    cols = con.shape[0]
    half = out.shape[2]
    vb, w, part = acc.shape[1], acc.shape[2], acc.shape[3]
    step = rows // CHUNKS
    cstep = cols // CHUNKS
    cut = depth // CUTS
    bits = PARTS * CUTS
    end = zl == zh
    mid = zl != zh

    def at(fc, fy, fl, fh):
        return (x, flip(core, fc) + 2 * flip(y, fy) + 4 * flip(zl, fl) + 8 * flip(zh, fh))

    def remote(src, dst, s, r, dev):
        return pltpu.make_async_remote_copy(
            src_ref=src, dst_ref=dst, send_sem=s, recv_sem=r, device_id=dev, device_id_type=MESH
        )

    def arows(k):
        return pl.ds(pl.multiple_of(k * step, step), step)

    def brows(k):
        return pl.ds(pl.multiple_of(k * cstep, cstep), cstep)

    sibling, beside, near = at(1, 0, 0, 0), at(0, 1, 0, 0), at(0, 0, 1, 0)
    far, across = at(0, 0, 0, 1), at(0, 0, 1, 1)
    a1 = remote(raw.at[0], raw.at[1], a1s.at[0], a1r.at[0], sibling)

    def b1(k):
        return remote(bb.at[0, brows(k)], bb.at[1, brows(k)], b1s.at[k], b1r.at[k], beside)

    def a2(k):
        return remote(raw.at[0, arows(k)], raw.at[2, arows(k)], a2s.at[k], a2r.at[k], near)

    def a3(k):
        return remote(raw.at[2, arows(k)], raw.at[3, arows(k)], a3s.at[k], a3r.at[k], sibling)

    def bit(b, k):
        lines = pl.ds(pl.multiple_of((k // CUTS) * part, part), part)
        lanes = pl.ds(pl.multiple_of((k % CUTS) * cut, cut), cut)
        return bb.at[b, lines, lanes]

    def b2(k):
        return remote(bit(0, k), bit(2, k), b2s.at[k], b2r.at[k], far)

    def b2pass(k):
        return remote(bit(4, k), bit(2, k), b2s.at[k], b2r.at[k], near)

    def b3(k):
        return remote(bit(2, k), bit(3, k), b3s.at[k], b3r.at[k], beside)

    def b5(j):
        k = bits - TWICE + j
        return remote(bit(1, k), bit(3, k), b5s.at[j], b3r.at[k], far)

    def b4(k):
        return remote(bb.at[0, brows(k)], bb.at[4, brows(k)], b4s.at[k], b4r.at[k], across)

    def b4_end(i):
        low = cols - LAST
        lines = pl.ds(cols - cstep, cstep - LAST) if i == 0 else pl.ds(low, LAST)
        lanes = pl.ds(0, depth) if i == 0 else pl.ds((i - 1) * (depth // 2), depth // 2)
        t = CHUNKS - 1 + i
        return remote(bb.at[0, lines, lanes], bb.at[4, lines, lanes], b4s.at[t], b4r.at[t], across)

    def slot(a, b, h):
        return (b * SIDE + a) * PARTS + h

    def xcopy(t):
        return remote(xs.at[t], xr.at[t], xss.at[t], xsr.at[t], (1 - x, me))

    def zcopy(t, a):
        return remote(zs.at[t], zr.at[t], zss.at[t], zsr.at[t], at(a % 2, 0, a // 2, 0))

    def each(n, fn, lo=0):
        def run(k, carry):
            fn(k)
            return carry
        lax.fori_loop(lo, n, run, 0)

    def active(a, b):
        kept = jnp.logical_and(b == 4, jnp.logical_and(mid, a < 2))
        shared = jnp.logical_and(b == 2, jnp.logical_or(mid, a < 2))
        return jnp.logical_or(jnp.logical_or(kept, shared), jnp.logical_and(b != 2, b != 4))

    def returned(a, b):
        kept = jnp.logical_and(b == 4, jnp.logical_and(mid, a < 2))
        shared = jnp.logical_and(b == 2, jnp.logical_or(end, a < 2))
        return jnp.logical_or(jnp.logical_or(kept, shared), jnp.logical_and(b != 2, b != 4))

    def owner(a, b):
        fy = jnp.where(b == 4, 0, b % 2)
        fl = jnp.where(b == 4, 1, 0)
        fh = jnp.where(b >= 2, 1, 0)
        return (
            flip(core, a % 2) + 2 * flip(y, fy) + 4 * flip(flip(zl, a // 2), fl) + 8 * flip(zh, fh)
        )

    lines = 16

    def screen(a, r):
        scr[a, r, :] = (raw[a, r, :].astype(jnp.float32) * scr_row[...]).astype(jnp.bfloat16)

    def blank(t):
        acc[t] = jnp.zeros((vb, w, part), jnp.float32)

    def screen_all(a):
        each(rows // lines, lambda i: screen(a, pl.ds(pl.multiple_of(i * lines, lines), lines)))

    barrier = pltpu.get_barrier_semaphore()
    greeted = (near, beside, (1 - x, me), sibling)

    @pl.when(mid)
    def _():
        pl.semaphore_signal(barrier, inc=1, device_id=across, device_id_type=MESH)

    for dev in greeted:
        pl.semaphore_signal(barrier, inc=1, device_id=dev, device_id_type=MESH)
    def own_a(k):
        return pltpu.make_async_copy(val.at[arows(k)], raw.at[0, arows(k)], loc.at[k])

    def own_b(k):
        return pltpu.make_async_copy(con.at[brows(k)], bb.at[0, brows(k)], loc.at[CHUNKS + k])

    own_row = pltpu.make_async_copy(scr_in, scr_row, loc.at[2 * CHUNKS])

    def fetch(k):
        own_b(k).start()
        own_a(k).start()

    each(CHUNKS, fetch)
    own_row.start()
    pl.semaphore_wait(barrier, len(greeted) + jnp.where(mid, 1, 0))

    def open_streams(k):
        own_b(k).wait()

        @pl.when(jnp.logical_and(mid, k < CHUNKS - 1))
        def _():
            b4(k).start()

        @pl.when(jnp.logical_and(mid, k == CHUNKS - 1))
        def _():
            for i in range(3):
                b4_end(i).start()

        b1(k).start()
        own_a(k).wait()
        a2(k).start()

    each(CHUNKS, open_streams)
    a1.start()
    own_row.wait()
    screen_all(0)
    each(2 * SIDE * PARTS, lambda i: blank(2 * SIDE * PARTS + i))

    def send(a, b, h):
        @pl.when(active(a, b))
        def _():
            t = slot(a, b, h)
            other = pl.ds(pl.multiple_of((1 - x) * half, half), half)
            xs[t] = acc[t, :, other, :].astype(jnp.bfloat16)
            xcopy(t).start()

    def whole(a, b):
        @pl.when(active(a, b))
        def _():
            prod = lax.dot_general(
                scr[a], bb[b], (((1,), (1,)), ((), ())), preferred_element_type=jnp.float32
            )
            for h in range(PARTS):
                acc[slot(a, b, h)] = prod[:, h * part:(h + 1) * part].reshape(vb, w, part)
        each(PARTS, lambda h: send(a, b, h))

    def grow(b, k):
        h, q = k // CUTS, k % CUTS
        lanes = pl.ds(pl.multiple_of(q * cut, cut), cut)
        lines = pl.ds(pl.multiple_of(h * part, part), part)

        def one(i):
            a = SIDE - 1 - i

            @pl.when(active(a, b))
            def _():
                prod = lax.dot_general(
                    scr[a, :, lanes], bb[b, lines, lanes],
                    (((1,), (1,)), ((), ())), preferred_element_type=jnp.float32,
                )
                t = slot(a, b, h)
                acc[t] = acc[t] + prod.reshape(vb, w, part)

            @pl.when(q == CUTS - 1)
            def _():
                send(a, b, h)

        each(SIDE, one)

    def place(a, b, h, value):
        lanes = pl.ds(pl.multiple_of(h * part, part), part)
        out[:, pl.ds(owner(a, b), 1), :, lanes] = value[:, None]

    def drain(a, b, h):
        @pl.when(active(a, b))
        def _():
            t = slot(a, b, h)
            xcopy(t).wait_recv()
            mine = pl.ds(pl.multiple_of(x * half, half), half)
            total = acc[t, :, mine, :] + xr[t].astype(jnp.float32)

            @pl.when(a == 0)
            def _():
                place(0, b, h, total)

            @pl.when(a > 0)
            def _():
                zs[t] = total.astype(jnp.bfloat16)
                zcopy(t, a).start()

    def land(a, b, h):
        @pl.when(returned(a, b))
        def _():
            t = slot(a, b, h)
            zcopy(t, a).wait_recv()
            place(a, b, h, zr[t].astype(jnp.float32))

    whole(0, 0)
    a1.wait_recv()
    screen_all(1)
    whole(1, 0)

    ready = CHUNKS // PARTS

    def first(k):
        @pl.when(jnp.logical_and(mid, k == CHUNKS - 1))
        def _():
            each(CHUNKS - 1, lambda i: b4(i).wait_send())
            b4_end(0).wait_send()
            b4_end(1).wait_send()
            for dev in (near, at(1, 0, 1, 0)):
                pl.semaphore_signal(gate, inc=1, device_id=dev, device_id_type=MESH)
            b4_end(2).wait_send()

        @pl.when(jnp.logical_and(end, k == CHUNKS - 1))
        def _():
            pl.semaphore_wait(gate, 2)
            each(bits, lambda i: b2(i).start())

        a2(k).wait_recv()
        a3(k).start()

        @pl.when(mid)
        def _():
            @pl.when(k < CHUNKS - 1)
            def _():
                b4(k).wait_recv()

            @pl.when(k == CHUNKS - 1)
            def _():
                for i in range(3):
                    b4_end(i).wait_recv()

            @pl.when(k % ready == ready - 1)
            def _():
                each(CUTS, lambda i: b2pass((k // ready) * CUTS + i).start())

        screen(2, arows(k))

        @pl.when(k > 0)
        def _():
            a3(k - 1).wait_recv()
            screen(3, arows(k - 1))

    each(CHUNKS, first)
    a3(CHUNKS - 1).wait_recv()
    screen(3, arows(CHUNKS - 1))
    each(PARTS * 2, lambda i: drain(1 - i // PARTS, 0, i % PARTS))
    each(CHUNKS, lambda k: b1(k).wait_recv())

    @pl.when(end)
    def _():
        each(TWICE, lambda j: b5(j).start())

    def crosses(k):
        return jnp.logical_or(end, k < bits - TWICE)

    turns = 2 * SIDE
    lag = 2

    def early(i):
        j = i - 2
        a = jnp.where(i < 2, i, jnp.where(j < 2, 2 + j, j - 2))
        b = jnp.where(i < 2, 4, jnp.where(j < 2, 0, 1))
        return a, b

    def between(lo, k, hi):
        return jnp.logical_and(k >= lo, k < hi)

    def tail(k):
        b3(k).wait_recv()
        grow(3, k)

    def second(k):
        b2(k).wait_recv()

        @pl.when(crosses(k))
        def _():
            b3(k).start()

        grow(2, k)

        @pl.when(k < turns)
        def _():
            whole(*early(k))

        @pl.when(k >= lag)
        def _():
            tail(k - lag)

        @pl.when(between(lag, k, turns + lag))
        def _():
            a, b = early(k - lag)
            each(PARTS, lambda h: drain(a, b, h))

        @pl.when(between(CUTS + lag, k, CUTS + lag + SIDE))
        def _():
            drain(SIDE - 1 - (k - CUTS - lag), 2, 0)

        @pl.when(k >= bits - SIDE)
        def _():
            drain(bits - 1 - k, 3, 0)

        @pl.when(k >= bits - 6)
        def _():
            i = k - bits + 6
            land(1, jnp.where(i < 4, i // 2, 4), i % 2)

    each(bits, second)
    tail(bits - 2)
    each(SIDE, lambda i: drain(SIDE - 1 - i, 2, 1))
    tail(bits - 1)

    def arrive(lo, h):
        def one(j):
            land(2 + j % 2, lo + j // 2, h)
        return one

    land(1, 2, 0)
    land(1, 3, 0)
    each(4, arrive(0, 0))
    each(4, arrive(0, 1))
    each(SIDE, lambda i: drain(SIDE - 1 - i, 3, 1))
    each(4, arrive(2, 0))
    land(1, 2, 1)
    each(4, arrive(2, 1))
    land(1, 3, 1)

    a1.wait_send()

    def sent(k):
        a2(k).wait_send()
        a3(k).wait_send()
        b1(k).wait_send()
    each(CHUNKS, sent)

    def cleared(k):
        b2(k).wait_send()

        @pl.when(crosses(k))
        def _():
            b3(k).wait_send()
    each(bits, cleared)

    @pl.when(end)
    def _():
        each(TWICE, lambda j: b5(j).wait_send())

    def passed(i):
        a, b, h = (i // PARTS) % SIDE, i // (PARTS * SIDE), i % PARTS

        @pl.when(active(a, b))
        def _():
            xcopy(i).wait_send()

            @pl.when(a > 0)
            def _():
                zcopy(i, a).wait_send()
    each(BLOCKS * SIDE * PARTS, passed)


def grid_body(valence_pairs, conduction_pairs, screening):
    vb, w, depth = valence_pairs.shape
    bands, conduction, _ = conduction_pairs.shape
    cols = bands * conduction
    rows = vb * w
    half = w // lax.axis_size("pw")
    total_c = bands * lax.axis_size("pair")
    tiles = BLOCKS * SIDE * PARTS
    part = cols // PARTS
    bits = PARTS * CUTS
    dma = pltpu.SemaphoreType.DMA
    bf16 = jnp.bfloat16
    return pl.pallas_call(
        grid_kernel,
        out_shape=pltpu.VMEM((vb, total_c, half, conduction), jnp.float32),
        in_specs=[
            pl.BlockSpec(memory_space=pl.ANY),
            pl.BlockSpec(memory_space=pl.ANY),
            pl.BlockSpec(memory_space=pl.ANY),
        ],
        out_specs=pl.BlockSpec(memory_space=pltpu.VMEM),
        scratch_shapes=[
            pltpu.VMEM((1, depth), jnp.float32),
            pltpu.VMEM((SIDE, rows, depth), bf16),
            pltpu.VMEM((SIDE, rows, depth), bf16),
            pltpu.VMEM((BLOCKS, cols, depth), bf16),
            pltpu.VMEM((tiles, vb, w, part), jnp.float32),
            pltpu.VMEM((tiles, vb, half, part), bf16),
            pltpu.VMEM((tiles, vb, half, part), bf16),
            pltpu.VMEM((tiles, vb, half, part), bf16),
            pltpu.VMEM((tiles, vb, half, part), bf16),
            dma((2 * CHUNKS + 1,)),
            dma((1,)), dma((1,)),
            dma((CHUNKS,)), dma((CHUNKS,)), dma((CHUNKS,)), dma((CHUNKS,)),
            dma((CHUNKS,)), dma((CHUNKS,)),
            dma((bits,)), dma((bits,)), dma((bits,)), dma((bits,)),
            dma((CHUNKS + 2,)), dma((CHUNKS + 2,)),
            dma((TWICE,)),
            pltpu.SemaphoreType.REGULAR,
            dma((tiles,)), dma((tiles,)), dma((tiles,)), dma((tiles,)),
        ],
        compiler_params=pltpu.CompilerParams(
            collective_id=0, has_side_effects=True, vmem_limit_bytes=56 * 1024 * 1024
        ),
    )(
        valence_pairs.reshape(rows, depth),
        conduction_pairs.reshape(cols, depth),
        screening.reshape(1, depth),
    )


def solution(mesh):
    placed = (P("pair", None, "pw"), P("pair", None, "pw"), P("pw"))
    squared = mesh.shape["pw"] == 2 and mesh.shape["pair"] == SIDE * SIDE

    def body(valence_pairs, conduction_pairs, screening):
        if squared and conduction_pairs.shape[0] == 1:
            return grid_body(valence_pairs, conduction_pairs, screening)
        return general_body(valence_pairs, conduction_pairs, screening)

    return jax.shard_map(
        body, mesh=mesh, in_specs=placed, out_specs=P("pair", None, "pw", None), check_vma=False
    )
```

```python
import functools

import jax
import jax.numpy as jnp
from jax import lax
from jax.experimental import pallas as pl
from jax.experimental.pallas import tpu as pltpu
from jax.sharding import PartitionSpec as P

MESH = pl.DeviceIdType.MESH
SIDE = 4
CHUNKS = 4
BLOCKS = 5
CUTS = 8
TWICE = 1
LAST = 16
PARTS = 2


def contract(piece, flat_right, band_dev, conduction):
    first, second, width = piece.shape
    product = lax.dot_general(
        piece.reshape(first * second, width),
        flat_right,
        (((1,), (1,)), ((), ())),
        preferred_element_type=jnp.float32,
    )
    return product.reshape(first, second, band_dev, conduction)


def general_body(valence_pairs, conduction_pairs, screening):
    screened = (valence_pairs.astype(jnp.float32) * screening[None, None, :]).astype(jnp.bfloat16)
    band_dev, conduction, plane_dev = conduction_pairs.shape
    flat_local = conduction_pairs.reshape(band_dev * conduction, plane_dev)
    partial_value = contract(
        lax.all_gather(screened, "pair", axis=0, tiled=True), flat_local, band_dev, conduction
    )
    terms = lax.psum_scatter(partial_value, "pw", scatter_dimension=1, tiled=True)
    owned = lax.all_to_all(terms, "pair", split_axis=0, concat_axis=2, tiled=True)
    return owned.transpose(0, 2, 1, 3)


def flip(bit, by):
    return bit + by - 2 * bit * by


def grid_kernel(
    val, con, scr_in, out, scr_row, raw, scr, bb, acc, xs, xr, zs, zr,
    loc, a1s, a1r, a2s, a2r, a3s, a3r, b1s, b1r, b2s, b2r, b3s, b3r, b4s, b4r, b5s, gate, xss, xsr, zss, zsr,
):
    me, x = lax.axis_index("pair"), lax.axis_index("pw")
    core, y, zl, zh = me % 2, (me // 2) % 2, (me // 4) % 2, me // 8
    rows, depth = val.shape
    cols = con.shape[0]
    half = out.shape[2]
    vb, w, part = acc.shape[1], acc.shape[2], acc.shape[3]
    step = rows // CHUNKS
    cstep = cols // CHUNKS
    cut = depth // CUTS
    bits = PARTS * CUTS
    end = zl == zh
    mid = zl != zh

    def at(fc, fy, fl, fh):
        return (x, flip(core, fc) + 2 * flip(y, fy) + 4 * flip(zl, fl) + 8 * flip(zh, fh))

    def remote(src, dst, s, r, dev):
        return pltpu.make_async_remote_copy(
            src_ref=src, dst_ref=dst, send_sem=s, recv_sem=r, device_id=dev, device_id_type=MESH
        )

    def arows(k):
        return pl.ds(pl.multiple_of(k * step, step), step)

    def brows(k):
        return pl.ds(pl.multiple_of(k * cstep, cstep), cstep)

    sibling, beside, near = at(1, 0, 0, 0), at(0, 1, 0, 0), at(0, 0, 1, 0)
    far, across = at(0, 0, 0, 1), at(0, 0, 1, 1)
    a1 = remote(raw.at[0], raw.at[1], a1s.at[0], a1r.at[0], sibling)

    def b1(k):
        return remote(bb.at[0, brows(k)], bb.at[1, brows(k)], b1s.at[k], b1r.at[k], beside)

    def a2(k):
        return remote(raw.at[0, arows(k)], raw.at[2, arows(k)], a2s.at[k], a2r.at[k], near)

    def a3(k):
        return remote(raw.at[2, arows(k)], raw.at[3, arows(k)], a3s.at[k], a3r.at[k], sibling)

    def bit(b, k):
        lines = pl.ds(pl.multiple_of((k // CUTS) * part, part), part)
        lanes = pl.ds(pl.multiple_of((k % CUTS) * cut, cut), cut)
        return bb.at[b, lines, lanes]

    def b2(k):
        return remote(bit(0, k), bit(2, k), b2s.at[k], b2r.at[k], far)

    def b2pass(k):
        return remote(bit(4, k), bit(2, k), b2s.at[k], b2r.at[k], near)

    def b3(k):
        return remote(bit(2, k), bit(3, k), b3s.at[k], b3r.at[k], beside)

    def b5(j):
        k = bits - TWICE + j
        return remote(bit(1, k), bit(3, k), b5s.at[j], b3r.at[k], far)

    def b4(k):
        return remote(bb.at[0, brows(k)], bb.at[4, brows(k)], b4s.at[k], b4r.at[k], across)

    def b4_end(i):
        low = cols - LAST
        lines = pl.ds(cols - cstep, cstep - LAST) if i == 0 else pl.ds(low, LAST)
        lanes = pl.ds(0, depth) if i == 0 else pl.ds((i - 1) * (depth // 2), depth // 2)
        t = CHUNKS - 1 + i
        return remote(bb.at[0, lines, lanes], bb.at[4, lines, lanes], b4s.at[t], b4r.at[t], across)

    def slot(a, b, h):
        return (b * SIDE + a) * PARTS + h

    def xcopy(t):
        return remote(xs.at[t], xr.at[t], xss.at[t], xsr.at[t], (1 - x, me))

    def zcopy(t, a):
        return remote(zs.at[t], zr.at[t], zss.at[t], zsr.at[t], at(a % 2, 0, a // 2, 0))

    def each(n, fn, lo=0):
        def run(k, carry):
            fn(k)
            return carry
        lax.fori_loop(lo, n, run, 0)

    def active(a, b):
        kept = jnp.logical_and(b == 4, jnp.logical_and(mid, a < 2))
        shared = jnp.logical_and(b == 2, jnp.logical_or(mid, a < 2))
        return jnp.logical_or(jnp.logical_or(kept, shared), jnp.logical_and(b != 2, b != 4))

    def returned(a, b):
        kept = jnp.logical_and(b == 4, jnp.logical_and(mid, a < 2))
        shared = jnp.logical_and(b == 2, jnp.logical_or(end, a < 2))
        return jnp.logical_or(jnp.logical_or(kept, shared), jnp.logical_and(b != 2, b != 4))

    def owner(a, b):
        fy = jnp.where(b == 4, 0, b % 2)
        fl = jnp.where(b == 4, 1, 0)
        fh = jnp.where(b >= 2, 1, 0)
        return (
            flip(core, a % 2) + 2 * flip(y, fy) + 4 * flip(flip(zl, a // 2), fl) + 8 * flip(zh, fh)
        )

    lines = 16

    def screen(a, r):
        scr[a, r, :] = (raw[a, r, :].astype(jnp.float32) * scr_row[...]).astype(jnp.bfloat16)

    def blank(t):
        acc[t] = jnp.zeros((vb, w, part), jnp.float32)

    def screen_all(a):
        each(rows // lines, lambda i: screen(a, pl.ds(pl.multiple_of(i * lines, lines), lines)))

    barrier = pltpu.get_barrier_semaphore()
    greeted = (near, beside, (1 - x, me), sibling)

    @pl.when(mid)
    def _():
        pl.semaphore_signal(barrier, inc=1, device_id=across, device_id_type=MESH)

    for dev in greeted:
        pl.semaphore_signal(barrier, inc=1, device_id=dev, device_id_type=MESH)
    def own_a(k):
        return pltpu.make_async_copy(val.at[arows(k)], raw.at[0, arows(k)], loc.at[k])

    def own_b(k):
        return pltpu.make_async_copy(con.at[brows(k)], bb.at[0, brows(k)], loc.at[CHUNKS + k])

    own_row = pltpu.make_async_copy(scr_in, scr_row, loc.at[2 * CHUNKS])

    def fetch(k):
        own_b(k).start()
        own_a(k).start()

    each(CHUNKS, fetch)
    own_row.start()
    pl.semaphore_wait(barrier, len(greeted) + jnp.where(mid, 1, 0))

    def open_streams(k):
        own_b(k).wait()

        @pl.when(jnp.logical_and(mid, k < CHUNKS - 1))
        def _():
            b4(k).start()

        @pl.when(jnp.logical_and(mid, k == CHUNKS - 1))
        def _():
            for i in range(3):
                b4_end(i).start()

        b1(k).start()
        own_a(k).wait()
        a2(k).start()

    each(CHUNKS, open_streams)
    a1.start()
    own_row.wait()
    screen_all(0)
    each(2 * SIDE * PARTS, lambda i: blank(2 * SIDE * PARTS + i))

    def send(a, b, h):
        @pl.when(active(a, b))
        def _():
            t = slot(a, b, h)
            other = pl.ds(pl.multiple_of((1 - x) * half, half), half)
            xs[t] = acc[t, :, other, :].astype(jnp.bfloat16)
            xcopy(t).start()

    def whole(a, b):
        @pl.when(active(a, b))
        def _():
            prod = lax.dot_general(
                scr[a], bb[b], (((1,), (1,)), ((), ())), preferred_element_type=jnp.float32
            )
            for h in range(PARTS):
                acc[slot(a, b, h)] = prod[:, h * part:(h + 1) * part].reshape(vb, w, part)
        each(PARTS, lambda h: send(a, b, h))

    def grow(b, k):
        h, q = k // CUTS, k % CUTS
        lanes = pl.ds(pl.multiple_of(q * cut, cut), cut)
        lines = pl.ds(pl.multiple_of(h * part, part), part)

        def one(i):
            a = SIDE - 1 - i

            @pl.when(active(a, b))
            def _():
                prod = lax.dot_general(
                    scr[a, :, lanes], bb[b, lines, lanes],
                    (((1,), (1,)), ((), ())), preferred_element_type=jnp.float32,
                )
                t = slot(a, b, h)
                acc[t] = acc[t] + prod.reshape(vb, w, part)

            @pl.when(q == CUTS - 1)
            def _():
                send(a, b, h)

        each(SIDE, one)

    def place(a, b, h, value):
        lanes = pl.ds(pl.multiple_of(h * part, part), part)
        out[:, pl.ds(owner(a, b), 1), :, lanes] = value[:, None]

    def drain(a, b, h):
        @pl.when(active(a, b))
        def _():
            t = slot(a, b, h)
            xcopy(t).wait_recv()
            mine = pl.ds(pl.multiple_of(x * half, half), half)
            total = acc[t, :, mine, :] + xr[t].astype(jnp.float32)

            @pl.when(a == 0)
            def _():
                place(0, b, h, total)

            @pl.when(a > 0)
            def _():
                zs[t] = total.astype(jnp.bfloat16)
                zcopy(t, a).start()

    def land(a, b, h):
        @pl.when(returned(a, b))
        def _():
            t = slot(a, b, h)
            zcopy(t, a).wait_recv()
            place(a, b, h, zr[t].astype(jnp.float32))

    whole(0, 0)
    a1.wait_recv()
    screen_all(1)
    whole(1, 0)

    ready = CHUNKS // PARTS

    def first(k):
        @pl.when(jnp.logical_and(mid, k == CHUNKS - 1))
        def _():
            each(CHUNKS - 1, lambda i: b4(i).wait_send())
            b4_end(0).wait_send()
            b4_end(1).wait_send()
            for dev in (near, at(1, 0, 1, 0)):
                pl.semaphore_signal(gate, inc=1, device_id=dev, device_id_type=MESH)
            b4_end(2).wait_send()

        @pl.when(jnp.logical_and(end, k == CHUNKS - 1))
        def _():
            pl.semaphore_wait(gate, 2)
            each(bits, lambda i: b2(i).start())

        a2(k).wait_recv()
        a3(k).start()

        @pl.when(mid)
        def _():
            @pl.when(k < CHUNKS - 1)
            def _():
                b4(k).wait_recv()

            @pl.when(k == CHUNKS - 1)
            def _():
                for i in range(3):
                    b4_end(i).wait_recv()

            @pl.when(k % ready == ready - 1)
            def _():
                each(CUTS, lambda i: b2pass((k // ready) * CUTS + i).start())

        screen(2, arows(k))

        @pl.when(k > 0)
        def _():
            a3(k - 1).wait_recv()
            screen(3, arows(k - 1))

    each(CHUNKS, first)
    a3(CHUNKS - 1).wait_recv()
    screen(3, arows(CHUNKS - 1))
    each(PARTS * 2, lambda i: drain(1 - i // PARTS, 0, i % PARTS))
    each(CHUNKS, lambda k: b1(k).wait_recv())

    @pl.when(end)
    def _():
        each(TWICE, lambda j: b5(j).start())

    def crosses(k):
        return jnp.logical_or(end, k < bits - TWICE)

    turns = 2 * SIDE
    lag = 2

    def early(i):
        j = i - 2
        a = jnp.where(i < 2, i, jnp.where(j < 2, 2 + j, j - 2))
        b = jnp.where(i < 2, 4, jnp.where(j < 2, 0, 1))
        return a, b

    def between(lo, k, hi):
        return jnp.logical_and(k >= lo, k < hi)

    def tail(k):
        b3(k).wait_recv()
        grow(3, k)

    def second(k):
        b2(k).wait_recv()

        @pl.when(crosses(k))
        def _():
            b3(k).start()

        grow(2, k)

        @pl.when(k < turns)
        def _():
            whole(*early(k))

        @pl.when(k >= lag)
        def _():
            tail(k - lag)

        @pl.when(between(lag, k, turns + lag))
        def _():
            a, b = early(k - lag)
            each(PARTS, lambda h: drain(a, b, h))

        @pl.when(between(CUTS + lag, k, CUTS + lag + SIDE))
        def _():
            drain(SIDE - 1 - (k - CUTS - lag), 2, 0)

        @pl.when(k >= bits - SIDE)
        def _():
            drain(bits - 1 - k, 3, 0)

        @pl.when(k >= bits - 6)
        def _():
            i = k - bits + 6
            land(1, jnp.where(i < 4, i // 2, 4), i % 2)

    each(bits, second)
    tail(bits - 2)
    tail(bits - 1)

    def arrive(lo, h):
        def one(j):
            land(2 + j % 2, lo + j // 2, h)
        return one

    each(SIDE, lambda i: drain(SIDE - 1 - i, 2, 1))
    a1.wait_send()

    def sent(k):
        a2(k).wait_send()
        a3(k).wait_send()
        b1(k).wait_send()
    each(CHUNKS, sent)

    def cleared(k):
        b2(k).wait_send()

        @pl.when(crosses(k))
        def _():
            b3(k).wait_send()
    each(bits, cleared)

    @pl.when(end)
    def _():
        each(TWICE, lambda j: b5(j).wait_send())

    def passed(i):
        a, b, h = (i // PARTS) % SIDE, i // (PARTS * SIDE), i % PARTS

        @pl.when(active(a, b))
        def _():
            xcopy(i).wait_send()

            @pl.when(a > 0)
            def _():
                zcopy(i, a).wait_send()

    land(1, 2, 0)
    land(1, 3, 0)
    each(SIDE, lambda i: drain(SIDE - 1 - i, 3, 1))
    each(4, arrive(0, 0))
    each(4, arrive(0, 1))
    each(4, arrive(2, 0))
    land(1, 2, 1)
    each(2 * SIDE * PARTS, passed)
    each(BLOCKS * SIDE * PARTS, passed, 4 * SIDE * PARTS)

    each(4, arrive(2, 1))
    land(1, 3, 1)

    each(4 * SIDE * PARTS, passed, 2 * SIDE * PARTS)


def grid_body(valence_pairs, conduction_pairs, screening):
    vb, w, depth = valence_pairs.shape
    bands, conduction, _ = conduction_pairs.shape
    cols = bands * conduction
    rows = vb * w
    half = w // lax.axis_size("pw")
    total_c = bands * lax.axis_size("pair")
    tiles = BLOCKS * SIDE * PARTS
    part = cols // PARTS
    bits = PARTS * CUTS
    dma = pltpu.SemaphoreType.DMA
    bf16 = jnp.bfloat16
    return pl.pallas_call(
        grid_kernel,
        out_shape=pltpu.VMEM((vb, total_c, half, conduction), jnp.float32),
        in_specs=[
            pl.BlockSpec(memory_space=pl.ANY),
            pl.BlockSpec(memory_space=pl.ANY),
            pl.BlockSpec(memory_space=pl.ANY),
        ],
        out_specs=pl.BlockSpec(memory_space=pltpu.VMEM),
        scratch_shapes=[
            pltpu.VMEM((1, depth), jnp.float32),
            pltpu.VMEM((SIDE, rows, depth), bf16),
            pltpu.VMEM((SIDE, rows, depth), bf16),
            pltpu.VMEM((BLOCKS, cols, depth), bf16),
            pltpu.VMEM((tiles, vb, w, part), jnp.float32),
            pltpu.VMEM((tiles, vb, half, part), bf16),
            pltpu.VMEM((tiles, vb, half, part), bf16),
            pltpu.VMEM((tiles, vb, half, part), bf16),
            pltpu.VMEM((tiles, vb, half, part), bf16),
            dma((2 * CHUNKS + 1,)),
            dma((1,)), dma((1,)),
            dma((CHUNKS,)), dma((CHUNKS,)), dma((CHUNKS,)), dma((CHUNKS,)),
            dma((CHUNKS,)), dma((CHUNKS,)),
            dma((bits,)), dma((bits,)), dma((bits,)), dma((bits,)),
            dma((CHUNKS + 2,)), dma((CHUNKS + 2,)),
            dma((TWICE,)),
            pltpu.SemaphoreType.REGULAR,
            dma((tiles,)), dma((tiles,)), dma((tiles,)), dma((tiles,)),
        ],
        compiler_params=pltpu.CompilerParams(
            collective_id=0, has_side_effects=True, vmem_limit_bytes=56 * 1024 * 1024
        ),
    )(
        valence_pairs.reshape(rows, depth),
        conduction_pairs.reshape(cols, depth),
        screening.reshape(1, depth),
    )


def solution(mesh):
    placed = (P("pair", None, "pw"), P("pair", None, "pw"), P("pw"))
    squared = mesh.shape["pw"] == 2 and mesh.shape["pair"] == SIDE * SIDE

    def body(valence_pairs, conduction_pairs, screening):
        if squared and conduction_pairs.shape[0] == 1:
            return grid_body(valence_pairs, conduction_pairs, screening)
        return general_body(valence_pairs, conduction_pairs, screening)

    return jax.shard_map(
        body, mesh=mesh, in_specs=placed, out_specs=P("pair", None, "pw", None), check_vma=False
    )
```
